32 devices in a mesh: prow: 4 (over z), pcol: 8 (over y, x, core).
Axes of the slice: x: 2, y: 2, z: 4, core: 2. Of those that a mesh axis runs over, the one named last changes fastest.
Arguments:
- tiles: bfloat16 [4, 8, 32, 256, 256], P('prow', 'pcol')
- tile_brow: int32 [4, 8, 32], P('prow', 'pcol'), may hold values from 0 to 31, as said below
- tile_bcol: int32 [4, 8, 32], P('prow', 'pcol'), may hold values from 0 to 15, as said below
- tile_count: int32 [4, 8], P('prow', 'pcol'), may hold values from 8 to 32, as said below
Outputs:
- row_scale: float32 [32, 4, 256], P(None, 'prow')
- col_scale: float32 [16, 8, 256], P(None, 'pcol')
The draws below stay inside these ranges and needn't reach their ends.
Inputs may be any that keep to these rules, and one draw needn't show every extreme that they name: `tile_brow`: on one device, no two slots name the same pair of local block row and column; the diagonal tile of every block row is present and live, in the first slots of the device that holds it. `tile_bcol`: see tile_brow. `tile_count`: a device that holds diagonal tiles has all 32 slots live, every other device at most 16.
All inputs are finite; a program needn't handle non-finite values.
Results may differ from the reference program's by a relative error of at most 0.0003.
Values sent between devices are 32-bit elements; how exact they have to be, the bound alone decides.
A program may use at most 64 MiB of HBM per device.

```python
import jax
import jax.numpy as jnp
from jax import lax

TILE = 256
BR_DEV = 32
TILES_DEV = 32
SWEEPS = 3
BC_DEV = 16
N_PROW = 4
N_PCOL = 8


def draw_tiles(key, part):
    shape = (N_PROW, N_PCOL, TILES_DEV, TILE, TILE)
    base = jax.random.normal(jax.random.fold_in(key, 11), shape, jnp.float32)
    span = 2.3
    row_log = jax.random.uniform(jax.random.fold_in(key, 12), (N_PROW, N_PCOL, TILES_DEV, TILE, 1), jnp.float32, -span, span)
    col_log = jax.random.uniform(jax.random.fold_in(key, 13), (N_PROW, N_PCOL, TILES_DEV, 1, TILE), jnp.float32, -span, span)
    return (base * jnp.exp(row_log) * jnp.exp(col_log)).astype(jnp.bfloat16)


def place_slots(key):
    cells = BR_DEV * BC_DEV
    keys = jax.random.split(jax.random.fold_in(key, 21), N_PROW * N_PCOL)
    cell_ids = jnp.arange(cells, dtype=jnp.int32)
    rows_of = cell_ids // BC_DEV
    cols_of = cell_ids % BC_DEV

    def one_device(device_key, position):
        prow_id = position // N_PCOL
        pcol_id = position % N_PCOL
        diagonal = rows_of * N_PROW + prow_id == cols_of * N_PCOL + pcol_id
        order = jax.random.permutation(device_key, cells).astype(jnp.int32)
        score = jnp.where(diagonal, order - cells, order)
        chosen = jnp.argsort(score, stable=True)[:TILES_DEV].astype(jnp.int32)
        return (rows_of[chosen], cols_of[chosen])
    brows, bcols = jax.vmap(one_device)(keys, jnp.arange(N_PROW * N_PCOL, dtype=jnp.int32))
    return (brows.reshape(N_PROW, N_PCOL, TILES_DEV), bcols.reshape(N_PROW, N_PCOL, TILES_DEV))


def draw_tile_brow(key, part):
    return place_slots(key)[0].astype(jnp.int32)


def draw_tile_bcol(key, part):
    return place_slots(key)[1].astype(jnp.int32)


def draw_tile_count(key, part):
    low = max(TILES_DEV // 4, 1)
    high = max(TILES_DEV // 2, low)
    counts = jax.random.randint(jax.random.fold_in(key, 31), (N_PROW, N_PCOL), low, high + 1)
    prow_ids = jnp.arange(N_PROW, dtype=jnp.int32)[:, None]
    pcol_ids = jnp.arange(N_PCOL, dtype=jnp.int32)[None, :]
    holder = pcol_ids % N_PROW == prow_ids
    return jnp.where(holder, TILES_DEV, counts).astype(jnp.int32)


def setup_inputs(seed: int = 0) -> dict:
    key_list = jax.random.split(jax.random.key(seed), 5)
    return {
        "tiles": draw_tiles(jax.random.fold_in(key_list[4], 71), 0),
        "tile_brow": draw_tile_brow(jax.random.fold_in(key_list[4], 71), 0),
        "tile_bcol": draw_tile_bcol(jax.random.fold_in(key_list[4], 71), 0),
        "tile_count": draw_tile_count(jax.random.fold_in(key_list[4], 71), 0),
    }


def rescale(scale, largest):
    return scale / jnp.sqrt(largest)

def reference(tiles, tile_brow, tile_bcol, tile_count):
    live = (jnp.arange(TILES_DEV, dtype=jnp.int32)[None, None, :] < tile_count[:, :, None]).astype(jnp.float32)
    row_vec = jnp.ones((N_PROW, BR_DEV, TILE), jnp.float32)
    col_vec = jnp.ones((N_PCOL, BC_DEV, TILE), jnp.float32)
    col_ids = jnp.arange(N_PCOL, dtype=jnp.int32)[:, None]
    for sweep in range(SWEEPS):

        def one_row(inputs):
            block, brow, bcol, alive, rows = inputs
            row_take = rows[brow]
            col_take = col_vec[col_ids, bcol]
            scaled = jnp.abs(block.astype(jnp.float32)) * row_take[:, :, :, None] * col_take[:, :, None, :]
            row_part = lax.optimization_barrier(jnp.max(scaled, axis=3)) * alive[:, :, None]
            col_part = lax.optimization_barrier(jnp.max(scaled, axis=2)) * alive[:, :, None]
            row_new = jnp.zeros((BR_DEV, TILE), jnp.float32).at[brow.reshape(-1)].max(row_part.reshape(-1, TILE))
            col_new = jnp.zeros((N_PCOL, BC_DEV, TILE), jnp.float32).at[jnp.broadcast_to(col_ids, bcol.shape).reshape(-1), bcol.reshape(-1)].max(col_part.reshape(-1, TILE))
            return (row_new, col_new)
        row_max, col_parts = lax.map(one_row, (tiles, tile_brow, tile_bcol, live, row_vec))
        col_max = lax.optimization_barrier(jnp.max(col_parts, axis=0))
        row_vec = rescale(row_vec, row_max)
        col_vec = rescale(col_vec, col_max)
    return (jnp.transpose(row_vec, (1, 0, 2)), jnp.transpose(col_vec, (1, 0, 2)))
```

```python
import functools

import jax
import jax.numpy as jnp
from jax import lax
from jax.experimental import pallas as pl
from jax.experimental.pallas import tpu as pltpu
from jax.sharding import PartitionSpec as P

BR_DEV = 32
SWEEPS = 3
LANES = 128
LOADS = 8


def rescale(scale, largest):
    return scale / jnp.sqrt(largest)


def kernel(
    n_prow, n_pcol, col_blocks, slots, width,
    brow_ref, bcol_ref, count_ref, tiles_ref,
    row_out, col_out,
    block, row_split, col_vec, row_send, col_send, row_recv, col_recv,
    load_sem, row_send_sem, row_recv_sem, col_send_sem, col_recv_sem,
):
    per = slots // LOADS
    loads = [
        pltpu.make_async_copy(
            tiles_ref.at[pl.ds(i * per, per)], block.at[pl.ds(i * per, per)], load_sem.at[i]
        )
        for i in range(LOADS)
    ]
    for load in loads:
        load.start()

    pr = lax.axis_index("prow")
    pc = lax.axis_index("pcol")
    barrier = pltpu.get_barrier_semaphore()
    for d in range(1, n_pcol):
        pl.semaphore_signal(barrier, inc=1, device_id={"pcol": lax.rem(pc + d, n_pcol)})
    for d in range(1, n_prow):
        pl.semaphore_signal(barrier, inc=1, device_id={"prow": lax.rem(pr + d, n_prow)})

    count = count_ref[0]
    row_ids = lax.broadcasted_iota(jnp.int32, (BR_DEV, width), 0)
    col_ids = lax.broadcasted_iota(jnp.int32, (col_blocks, width), 0)
    lane_ids = lax.broadcasted_iota(jnp.int32, (1, LANES), 1)
    ones = jnp.ones((LANES, LANES), jnp.bfloat16)
    step = 16
    halves = width // LANES

    def one_tile(s, carry, first):
        row_acc, col_acc = carry
        brow = brow_ref[s]
        bcol = bcol_ref[s]
        if not first:
            pick = jnp.where(
                (lane_ids % BR_DEV == brow) & (lane_ids < 3 * BR_DEV), 1.0, 0.0
            ).astype(jnp.bfloat16)
            spread = jnp.dot(
                row_split[...] * pick, ones, preferred_element_type=jnp.float32
            )
            cols = col_vec[pl.ds(bcol, 1), :]
        col_part = [jnp.zeros((step, LANES), jnp.float32) for _ in range(halves)]
        pieces = []
        for g in range(width // step):
            best = None
            for h in range(halves):
                x = jnp.abs(
                    block[s, g * step:(g + 1) * step, h * LANES:(h + 1) * LANES].astype(jnp.float32)
                )
                if not first:
                    x = x * spread[g * step:(g + 1) * step]
                    x = x * cols[:, h * LANES:(h + 1) * LANES]
                col_part[h] = jnp.maximum(col_part[h], x)
                best = x if best is None else jnp.maximum(best, x)
            pieces.append(best)
        parts = []
        for h in range(halves):
            part = jnp.concatenate(pieces[h * LANES // step:(h + 1) * LANES // step], axis=0)
            parts.append(jnp.max(part.T, axis=0, keepdims=True))
        row_part = jnp.concatenate(parts, axis=1)
        col_top = jnp.concatenate([jnp.max(c, axis=0, keepdims=True) for c in col_part], axis=1)
        alive = s < count
        row_at = jnp.where(alive, brow, -1)
        col_at = jnp.where(alive, bcol, -1)
        row_acc = jnp.maximum(row_acc, jnp.where(row_ids == row_at, row_part, 0.0))
        col_acc = jnp.maximum(col_acc, jnp.where(col_ids == col_at, col_top, 0.0))
        return row_acc, col_acc

    row_vec = jnp.ones((BR_DEV, width), jnp.float32)
    col_now = jnp.ones((col_blocks, width), jnp.float32)
    for sweep in range(SWEEPS):
        carry = (
            jnp.zeros((BR_DEV, width), jnp.float32),
            jnp.zeros((col_blocks, width), jnp.float32),
        )
        body = functools.partial(one_tile, first=sweep == 0)
        if sweep == 0:
            for i in range(LOADS):
                loads[i].wait()
                carry = lax.fori_loop(i * per, (i + 1) * per, body, carry)
        else:
            carry = lax.fori_loop(0, slots, body, carry)
        row_max, col_max = carry
        col_send[sweep] = col_max
        row_send[sweep] = row_max
        if sweep == 0:
            pl.semaphore_wait(barrier, n_pcol - 1 + n_prow - 1)
        copies = []
        for d in range(1, n_prow):
            copies.append(pltpu.make_async_remote_copy(
                src_ref=col_send.at[sweep], dst_ref=col_recv.at[sweep, d - 1],
                send_sem=col_send_sem.at[sweep, d - 1], recv_sem=col_recv_sem.at[sweep, d - 1],
                device_id={"prow": lax.rem(pr + d, n_prow)},
            ))
        for d in range(1, n_pcol):
            copies.append(pltpu.make_async_remote_copy(
                src_ref=row_send.at[sweep], dst_ref=row_recv.at[sweep, d - 1],
                send_sem=row_send_sem.at[sweep, d - 1], recv_sem=row_recv_sem.at[sweep, d - 1],
                device_id={"pcol": lax.rem(pc + d, n_pcol)},
            ))
        for copy in copies:
            copy.start()
        for copy in copies:
            copy.wait()
        for d in range(1, n_prow):
            col_max = jnp.maximum(col_max, col_recv[sweep, d - 1])
        for d in range(1, n_pcol):
            row_max = jnp.maximum(row_max, row_recv[sweep, d - 1])
        row_vec = rescale(row_vec, row_max)
        col_now = rescale(col_now, col_max)
        if sweep + 1 < SWEEPS:
            col_vec[...] = col_now
            top = row_vec.astype(jnp.bfloat16).astype(jnp.float32)
            left = row_vec - top
            mid = left.astype(jnp.bfloat16).astype(jnp.float32)
            low = left - mid
            rest = jnp.zeros((LANES - 3 * BR_DEV, width), jnp.float32)
            stack = jnp.concatenate([top, mid, low, rest], axis=0)
            for h in range(halves):
                row_split[h * LANES:(h + 1) * LANES, :] = (
                    stack[:, h * LANES:(h + 1) * LANES].T.astype(jnp.bfloat16)
                )
    row_out[...] = row_vec
    col_out[...] = col_now


def solution(mesh):
    n_prow, n_pcol = mesh.shape["prow"], mesh.shape["pcol"]

    def on_device(tiles, tile_brow, tile_bcol, tile_count):
        slots, width = tiles.shape[2], tiles.shape[3]
        col_blocks = BR_DEV * n_prow // n_pcol
        smem = pl.BlockSpec(memory_space=pltpu.SMEM)
        vmem = pl.BlockSpec(memory_space=pltpu.VMEM)
        row_vec, col_vec = pl.pallas_call(
            functools.partial(kernel, n_prow, n_pcol, col_blocks, slots, width),
            out_shape=(
                jax.ShapeDtypeStruct((BR_DEV, width), jnp.float32),
                jax.ShapeDtypeStruct((col_blocks, width), jnp.float32),
            ),
            in_specs=[smem, smem, smem, pl.BlockSpec(memory_space=pl.ANY)],
            out_specs=(vmem, vmem),
            scratch_shapes=[
                pltpu.VMEM((slots, width, width), jnp.bfloat16),
                pltpu.VMEM((width, LANES), jnp.bfloat16),
                pltpu.VMEM((col_blocks, width), jnp.float32),
                pltpu.VMEM((SWEEPS, BR_DEV, width), jnp.float32),
                pltpu.VMEM((SWEEPS, col_blocks, width), jnp.float32),
                pltpu.VMEM((SWEEPS, n_pcol - 1, BR_DEV, width), jnp.float32),
                pltpu.VMEM((SWEEPS, n_prow - 1, col_blocks, width), jnp.float32),
                pltpu.SemaphoreType.DMA((LOADS,)),
                pltpu.SemaphoreType.DMA((SWEEPS, n_pcol - 1)),
                pltpu.SemaphoreType.DMA((SWEEPS, n_pcol - 1)),
                pltpu.SemaphoreType.DMA((SWEEPS, n_prow - 1)),
                pltpu.SemaphoreType.DMA((SWEEPS, n_prow - 1)),
            ],
            compiler_params=pltpu.CompilerParams(collective_id=0, has_side_effects=True),
        )(
            tile_brow.reshape(slots), tile_bcol.reshape(slots), tile_count.reshape(1),
            tiles.reshape(slots, width, width),
        )
        return (row_vec.reshape(BR_DEV, 1, width), col_vec.reshape(col_blocks, 1, width))

    return jax.shard_map(
        on_device,
        mesh=mesh,
        in_specs=(
            P("prow", "pcol", None, None, None),
            P("prow", "pcol", None),
            P("prow", "pcol", None),
            P("prow", "pcol"),
        ),
        out_specs=(P(None, "prow", None), P(None, "pcol", None)),
        check_vma=False,
    )
```

```python
import functools

import jax
import jax.numpy as jnp
from jax import lax
from jax.experimental import pallas as pl
from jax.experimental.pallas import tpu as pltpu
from jax.sharding import PartitionSpec as P

BR_DEV = 32
SWEEPS = 3
LANES = 128
STEP = 4
ROWS = 16


def rescale(scale, largest):
    return scale / jnp.sqrt(largest)


def kernel(
    n_prow, n_pcol, col_blocks, slots, width,
    brow_ref, bcol_ref, count_ref, tiles_ref,
    row_out, col_out,
    block, row_split, col_vec, spread_a, spread_b, peak_a, peak_b,
    row_send, pair_recv, half_send, half_recv, done_send, done_recv, col_send, col_recv,
    load_sem, pair_send_sem, pair_recv_sem, half_send_sem, half_recv_sem,
    done_send_sem, done_recv_sem, col_send_sem, col_recv_sem,
):
    def load(t):
        at = pl.ds(t * STEP, STEP)
        return pltpu.make_async_copy(tiles_ref.at[at], block.at[at], load_sem.at[t])

    for t in range(slots // STEP):
        load(t).start()

    pr = lax.axis_index("prow")
    pc = lax.axis_index("pcol")
    side = lax.rem(pc, 2)
    partner = pc + 1 - 2 * side
    barrier = pltpu.get_barrier_semaphore()
    pl.semaphore_signal(barrier, inc=1, device_id={"pcol": partner})
    for d in range(1, n_pcol // 2):
        pl.semaphore_signal(barrier, inc=1, device_id={"pcol": lax.rem(pc + 2 * d, n_pcol)})
    for d in range(1, n_prow):
        pl.semaphore_signal(barrier, inc=1, device_id={"prow": lax.rem(pr + d, n_prow)})

    count = count_ref[0]
    row_ids = lax.broadcasted_iota(jnp.int32, (BR_DEV, width), 0)
    col_ids = lax.broadcasted_iota(jnp.int32, (col_blocks, width), 0)
    lane_ids = lax.broadcasted_iota(jnp.int32, (1, LANES), 1)
    ones = jnp.ones((LANES, LANES), jnp.bfloat16)
    lane_full = lax.broadcasted_iota(jnp.int32, (8, LANES), 1)
    lane_group = lane_full // 8
    own_lane = lane_full % 8 == lax.broadcasted_iota(jnp.int32, (8, LANES), 0)
    halves = width // LANES
    peak_b[...] = jnp.zeros_like(peak_b)

    def spread_rows(s, out, j):
        brow = brow_ref[jnp.minimum(s, slots - 1)]
        pick = jnp.where(
            (lane_ids % BR_DEV == brow) & (lane_ids < 3 * BR_DEV), 1.0, 0.0
        ).astype(jnp.bfloat16)
        out[j] = jnp.dot(row_split[...] * pick, ones, preferred_element_type=jnp.float32)

    def scale_tile(s, spread, peak, j, col_acc):
        bcol = bcol_ref[s]
        if spread is not None:
            cols = col_vec[pl.ds(bcol, 1), :]
        col_part = [None] * halves
        for g in range(width // ROWS):
            at = slice(g * ROWS, (g + 1) * ROWS)
            best = None
            for h in range(halves):
                lanes = slice(h * LANES, (h + 1) * LANES)
                x = jnp.abs(block[s, at, lanes]).astype(jnp.float32)
                if spread is not None:
                    x = (x * spread[j, at, :]) * cols[:, lanes]
                col_part[h] = x if g == 0 else jnp.maximum(col_part[h], x)
                best = x if h == 0 else jnp.maximum(best, x)
            peak[j, at, :] = best
        top = jnp.concatenate([jnp.max(c, axis=0, keepdims=True) for c in col_part], axis=1)
        col_at = jnp.where(s < count, bcol, -1)
        return jnp.maximum(col_acc, jnp.where(col_ids == col_at, top, 0.0))

    def reduce_rows(s, peak, j, row_acc):
        parts = []
        for h in range(halves):
            packed = None
            for g in range(LANES // 8):
                at = h * LANES + 8 * g
                best = jnp.max(peak[j, at:at + 8, :], axis=1, keepdims=True)
                best = jnp.broadcast_to(best, (8, LANES))
                packed = best if g == 0 else jnp.where(lane_group == g, best, packed)
            parts.append(jnp.max(jnp.where(own_lane, packed, 0.0), axis=0, keepdims=True))
        row_at = jnp.where((s >= 0) & (s < count), brow_ref[jnp.maximum(s, 0)], -1)
        return jnp.maximum(
            row_acc, jnp.where(row_ids == row_at, jnp.concatenate(parts, axis=1), 0.0)
        )

    def four_tiles(t, carry, first):
        row_acc, col_acc = carry
        base = t * STEP
        if first:
            load(t).wait()
        for part in range(2):
            here, peak = (spread_a, peak_a) if part == 0 else (spread_b, peak_b)
            there, last = (spread_b, peak_b) if part == 0 else (spread_a, peak_a)
            s = base + 2 * part
            if not first:
                for j in range(2):
                    spread_rows(s + 2 + j, there, j)
            for j in range(2):
                row_acc = reduce_rows(s - 2 + j, last, j, row_acc)
            for j in range(2):
                col_acc = scale_tile(s + j, None if first else here, peak, j, col_acc)
        return row_acc, col_acc

    row_vec = jnp.ones((BR_DEV, width), jnp.float32)
    col_now = jnp.ones((col_blocks, width), jnp.float32)
    half = BR_DEV // 2
    for sweep in range(SWEEPS):
        if sweep > 0:
            for j in range(2):
                spread_rows(j, spread_a, j)
        row_max, col_max = lax.fori_loop(
            0, slots // STEP, functools.partial(four_tiles, first=sweep == 0),
            (jnp.zeros((BR_DEV, width), jnp.float32), jnp.zeros((col_blocks, width), jnp.float32)),
        )
        col_send[sweep] = col_max
        for j in range(2):
            row_max = reduce_rows(slots - 2 + j, peak_b, j, row_max)
        row_send[sweep, 0] = row_max[:half]
        row_send[sweep, 1] = row_max[half:]
        if sweep == 0:
            pl.semaphore_wait(barrier, n_pcol // 2 + n_prow - 1)
        pair = pltpu.make_async_remote_copy(
            src_ref=row_send.at[sweep, 1 - side], dst_ref=pair_recv.at[sweep],
            send_sem=pair_send_sem.at[sweep], recv_sem=pair_recv_sem.at[sweep],
            device_id={"pcol": partner},
        )
        pair.start()
        col_copies = []
        for d in range(1, n_prow):
            col_copies.append(pltpu.make_async_remote_copy(
                src_ref=col_send.at[sweep], dst_ref=col_recv.at[sweep, d - 1],
                send_sem=col_send_sem.at[sweep, d - 1], recv_sem=col_recv_sem.at[sweep, d - 1],
                device_id={"prow": lax.rem(pr + d, n_prow)},
            ))
        for copy in col_copies:
            copy.start()
        mine = row_send[sweep, side]
        pair.wait()
        mine = jnp.maximum(mine, pair_recv[sweep])
        half_send[sweep] = mine
        half_copies = []
        for d in range(1, n_pcol // 2):
            half_copies.append(pltpu.make_async_remote_copy(
                src_ref=half_send.at[sweep], dst_ref=half_recv.at[sweep, d - 1],
                send_sem=half_send_sem.at[sweep, d - 1], recv_sem=half_recv_sem.at[sweep, d - 1],
                device_id={"pcol": lax.rem(pc + 2 * d, n_pcol)},
            ))
        for copy in half_copies:
            copy.start()
        for d, copy in enumerate(half_copies):
            copy.wait()
            mine = jnp.maximum(mine, half_recv[sweep, d])
        done_send[sweep] = mine
        done = pltpu.make_async_remote_copy(
            src_ref=done_send.at[sweep], dst_ref=done_recv.at[sweep],
            send_sem=done_send_sem.at[sweep], recv_sem=done_recv_sem.at[sweep],
            device_id={"pcol": partner},
        )
        done.start()
        for d, copy in enumerate(col_copies):
            copy.wait()
            col_max = jnp.maximum(col_max, col_recv[sweep, d])
        col_now = rescale(col_now, col_max)
        done.wait()
        other = done_recv[sweep]
        row_max = jnp.concatenate(
            [jnp.where(side == 0, mine, other), jnp.where(side == 0, other, mine)], axis=0
        )
        row_vec = rescale(row_vec, row_max)
        if sweep + 1 < SWEEPS:
            col_vec[...] = col_now
            top = row_vec.astype(jnp.bfloat16).astype(jnp.float32)
            left = row_vec - top
            mid = left.astype(jnp.bfloat16).astype(jnp.float32)
            low = left - mid
            rest = jnp.zeros((LANES - 3 * BR_DEV, width), jnp.float32)
            stack = jnp.concatenate([top, mid, low, rest], axis=0)
            for h in range(halves):
                row_split[h * LANES:(h + 1) * LANES, :] = (
                    stack[:, h * LANES:(h + 1) * LANES].T.astype(jnp.bfloat16)
                )
    row_out[...] = row_vec
    col_out[...] = col_now


def spell(row_ref, col_ref, row_out, col_out):
    for ref, out in ((row_ref, row_out), (col_ref, col_out)):
        for i in range(ref.shape[0]):
            out[i] = ref[i:i + 1, :]


def solution(mesh):
    n_prow, n_pcol = mesh.shape["prow"], mesh.shape["pcol"]

    def on_device(tiles, tile_brow, tile_bcol, tile_count):
        slots, width = tiles.shape[2], tiles.shape[3]
        col_blocks = BR_DEV * n_prow // n_pcol
        half = BR_DEV // 2
        smem = pl.BlockSpec(memory_space=pltpu.SMEM)
        vmem = pl.BlockSpec(memory_space=pltpu.VMEM)
        row_vec, col_vec = pl.pallas_call(
            functools.partial(kernel, n_prow, n_pcol, col_blocks, slots, width),
            out_shape=(
                jax.ShapeDtypeStruct((BR_DEV, width), jnp.float32),
                jax.ShapeDtypeStruct((col_blocks, width), jnp.float32),
            ),
            in_specs=[smem, smem, smem, pl.BlockSpec(memory_space=pl.ANY)],
            out_specs=(vmem, vmem),
            scratch_shapes=[
                pltpu.VMEM((slots, width, width), jnp.bfloat16),
                pltpu.VMEM((width, LANES), jnp.bfloat16),
                pltpu.VMEM((col_blocks, width), jnp.float32),
                pltpu.VMEM((2, width, LANES), jnp.float32),
                pltpu.VMEM((2, width, LANES), jnp.float32),
                pltpu.VMEM((2, width, LANES), jnp.float32),
                pltpu.VMEM((2, width, LANES), jnp.float32),
                pltpu.VMEM((SWEEPS, 2, half, width), jnp.float32),
                pltpu.VMEM((SWEEPS, half, width), jnp.float32),
                pltpu.VMEM((SWEEPS, half, width), jnp.float32),
                pltpu.VMEM((SWEEPS, n_pcol // 2 - 1, half, width), jnp.float32),
                pltpu.VMEM((SWEEPS, half, width), jnp.float32),
                pltpu.VMEM((SWEEPS, half, width), jnp.float32),
                pltpu.VMEM((SWEEPS, col_blocks, width), jnp.float32),
                pltpu.VMEM((SWEEPS, n_prow - 1, col_blocks, width), jnp.float32),
                pltpu.SemaphoreType.DMA((slots // STEP,)),
                pltpu.SemaphoreType.DMA((SWEEPS,)),
                pltpu.SemaphoreType.DMA((SWEEPS,)),
                pltpu.SemaphoreType.DMA((SWEEPS, n_pcol // 2 - 1)),
                pltpu.SemaphoreType.DMA((SWEEPS, n_pcol // 2 - 1)),
                pltpu.SemaphoreType.DMA((SWEEPS,)),
                pltpu.SemaphoreType.DMA((SWEEPS,)),
                pltpu.SemaphoreType.DMA((SWEEPS, n_prow - 1)),
                pltpu.SemaphoreType.DMA((SWEEPS, n_prow - 1)),
            ],
            compiler_params=pltpu.CompilerParams(collective_id=0, has_side_effects=True),
        )(
            tile_brow.reshape(slots), tile_bcol.reshape(slots), tile_count.reshape(1),
            tiles.reshape(slots, width, width),
        )
        return pl.pallas_call(
            spell,
            out_shape=(
                jax.ShapeDtypeStruct((BR_DEV, 1, width), jnp.float32),
                jax.ShapeDtypeStruct((col_blocks, 1, width), jnp.float32),
            ),
            in_specs=[vmem, vmem],
            out_specs=(vmem, vmem),
        )(row_vec, col_vec)

    return jax.shard_map(
        on_device,
        mesh=mesh,
        in_specs=(
            P("prow", "pcol", None, None, None),
            P("prow", "pcol", None),
            P("prow", "pcol", None),
            P("prow", "pcol"),
        ),
        out_specs=(P(None, "prow", None), P(None, "pcol", None)),
        check_vma=False,
    )
```

```python
import functools

import jax
import jax.numpy as jnp
from jax import lax
from jax.experimental import pallas as pl
from jax.experimental.pallas import tpu as pltpu
from jax.sharding import PartitionSpec as P

BR_DEV = 32
SWEEPS = 3
LANES = 128
STEP = 4
ROWS = 16


def rescale(scale, largest):
    return scale / jnp.sqrt(largest)


def kernel(
    n_prow, n_pcol, col_blocks, slots, width,
    brow_ref, bcol_ref, count_ref, tiles_ref,
    row_out, col_out,
    block, row_split, col_vec, spread_a, spread_b, peak_a, peak_b,
    row_send, part_recv, done_send, done_recv, col_send, col_recv,
    load_sem, part_send_sem, part_recv_sem,
    done_send_sem, done_recv_sem, col_send_sem, col_recv_sem,
):
    def load(t):
        at = pl.ds(t * STEP, STEP)
        return pltpu.make_async_copy(tiles_ref.at[at], block.at[at], load_sem.at[t])

    for t in range(slots // STEP):
        load(t).start()

    pr = lax.axis_index("prow")
    pc = lax.axis_index("pcol")
    barrier = pltpu.get_barrier_semaphore()
    for d in range(1, n_pcol):
        pl.semaphore_signal(barrier, inc=1, device_id={"pcol": lax.rem(pc + d, n_pcol)})
    for d in range(1, n_prow):
        pl.semaphore_signal(barrier, inc=1, device_id={"prow": lax.rem(pr + d, n_prow)})

    count = count_ref[0]
    row_ids = lax.broadcasted_iota(jnp.int32, (BR_DEV, width), 0)
    col_ids = lax.broadcasted_iota(jnp.int32, (col_blocks, width), 0)
    lane_ids = lax.broadcasted_iota(jnp.int32, (1, LANES), 1)
    ones = jnp.ones((LANES, LANES), jnp.bfloat16)
    lane_full = lax.broadcasted_iota(jnp.int32, (8, LANES), 1)
    lane_group = lane_full // 8
    own_lane = lane_full % 8 == lax.broadcasted_iota(jnp.int32, (8, LANES), 0)
    halves = width // LANES
    peak_b[...] = jnp.zeros_like(peak_b)

    def spread_rows(s, out, j):
        brow = brow_ref[jnp.minimum(s, slots - 1)]
        pick = jnp.where(
            (lane_ids % BR_DEV == brow) & (lane_ids < 3 * BR_DEV), 1.0, 0.0
        ).astype(jnp.bfloat16)
        out[j] = jnp.dot(row_split[...] * pick, ones, preferred_element_type=jnp.float32)

    def scale_tile(s, spread, peak, j, col_acc):
        bcol = bcol_ref[s]
        if spread is not None:
            cols = col_vec[pl.ds(bcol, 1), :]
        col_part = [None] * halves
        for g in range(width // ROWS):
            at = slice(g * ROWS, (g + 1) * ROWS)
            best = None
            for h in range(halves):
                lanes = slice(h * LANES, (h + 1) * LANES)
                x = jnp.abs(block[s, at, lanes]).astype(jnp.float32)
                if spread is not None:
                    x = (x * spread[j, at, :]) * cols[:, lanes]
                col_part[h] = x if g == 0 else jnp.maximum(col_part[h], x)
                best = x if h == 0 else jnp.maximum(best, x)
            peak[j, at, :] = best
        top = jnp.concatenate([jnp.max(c, axis=0, keepdims=True) for c in col_part], axis=1)
        col_at = jnp.where(s < count, bcol, -1)
        return jnp.maximum(col_acc, jnp.where(col_ids == col_at, top, 0.0))

    def reduce_rows(s, peak, j, row_acc):
        parts = []
        for h in range(halves):
            packed = None
            for g in range(LANES // 8):
                at = h * LANES + 8 * g
                best = jnp.max(peak[j, at:at + 8, :], axis=1, keepdims=True)
                best = jnp.broadcast_to(best, (8, LANES))
                packed = best if g == 0 else jnp.where(lane_group == g, best, packed)
            parts.append(jnp.max(jnp.where(own_lane, packed, 0.0), axis=0, keepdims=True))
        row_at = jnp.where((s >= 0) & (s < count), brow_ref[jnp.maximum(s, 0)], -1)
        return jnp.maximum(
            row_acc, jnp.where(row_ids == row_at, jnp.concatenate(parts, axis=1), 0.0)
        )

    def four_tiles(t, carry, first):
        row_acc, col_acc = carry
        base = t * STEP
        if first:
            load(t).wait()
        for part in range(2):
            here, peak = (spread_a, peak_a) if part == 0 else (spread_b, peak_b)
            there, last = (spread_b, peak_b) if part == 0 else (spread_a, peak_a)
            s = base + 2 * part
            if not first:
                for j in range(2):
                    spread_rows(s + 2 + j, there, j)
            for j in range(2):
                row_acc = reduce_rows(s - 2 + j, last, j, row_acc)
            for j in range(2):
                col_acc = scale_tile(s + j, None if first else here, peak, j, col_acc)
        return row_acc, col_acc

    row_vec = jnp.ones((BR_DEV, width), jnp.float32)
    col_now = jnp.ones((col_blocks, width), jnp.float32)
    share = BR_DEV // n_pcol
    for sweep in range(SWEEPS):
        if sweep > 0:
            for j in range(2):
                spread_rows(j, spread_a, j)
        row_max, col_max = lax.fori_loop(
            0, slots // STEP, functools.partial(four_tiles, first=sweep == 0),
            (jnp.zeros((BR_DEV, width), jnp.float32), jnp.zeros((col_blocks, width), jnp.float32)),
        )
        col_send[sweep] = col_max
        for j in range(2):
            row_max = reduce_rows(slots - 2 + j, peak_b, j, row_max)
        row_send[sweep] = row_max
        if sweep == 0:
            pl.semaphore_wait(barrier, n_pcol - 1 + n_prow - 1)
        part_copies = []
        for d in range(1, n_pcol):
            to = lax.rem(pc + d, n_pcol)
            part_copies.append(pltpu.make_async_remote_copy(
                src_ref=row_send.at[sweep], dst_ref=part_recv.at[sweep, d - 1],
                send_sem=part_send_sem.at[sweep, d - 1], recv_sem=part_recv_sem.at[sweep, d - 1],
                device_id={"pcol": to},
            ))
        for copy in part_copies:
            copy.start()
        col_copies = []
        for d in range(1, n_prow):
            col_copies.append(pltpu.make_async_remote_copy(
                src_ref=col_send.at[sweep], dst_ref=col_recv.at[sweep, d - 1],
                send_sem=col_send_sem.at[sweep, d - 1], recv_sem=col_recv_sem.at[sweep, d - 1],
                device_id={"prow": lax.rem(pr + d, n_prow)},
            ))
        for copy in col_copies:
            copy.start()
        for d, copy in enumerate(col_copies):
            copy.wait()
            col_max = jnp.maximum(col_max, col_recv[sweep, d])
        col_now = rescale(col_now, col_max)
        for d, copy in enumerate(part_copies):
            copy.wait()
            row_max = jnp.maximum(row_max, part_recv[sweep, d])
        row_vec = rescale(row_vec, row_max)
        if sweep + 1 < SWEEPS:
            col_vec[...] = col_now
            top = row_vec.astype(jnp.bfloat16).astype(jnp.float32)
            left = row_vec - top
            mid = left.astype(jnp.bfloat16).astype(jnp.float32)
            low = left - mid
            rest = jnp.zeros((LANES - 3 * BR_DEV, width), jnp.float32)
            stack = jnp.concatenate([top, mid, low, rest], axis=0)
            for h in range(halves):
                row_split[h * LANES:(h + 1) * LANES, :] = (
                    stack[:, h * LANES:(h + 1) * LANES].T.astype(jnp.bfloat16)
                )
    row_out[...] = row_vec
    col_out[...] = col_now


def spell(row_ref, col_ref, row_out, col_out):
    for ref, out in ((row_ref, row_out), (col_ref, col_out)):
        for i in range(ref.shape[0]):
            out[i] = ref[i:i + 1, :]


def solution(mesh):
    n_prow, n_pcol = mesh.shape["prow"], mesh.shape["pcol"]

    def on_device(tiles, tile_brow, tile_bcol, tile_count):
        slots, width = tiles.shape[2], tiles.shape[3]
        col_blocks = BR_DEV * n_prow // n_pcol
        share = BR_DEV // n_pcol
        smem = pl.BlockSpec(memory_space=pltpu.SMEM)
        vmem = pl.BlockSpec(memory_space=pltpu.VMEM)
        row_vec, col_vec = pl.pallas_call(
            functools.partial(kernel, n_prow, n_pcol, col_blocks, slots, width),
            out_shape=(
                jax.ShapeDtypeStruct((BR_DEV, width), jnp.float32),
                jax.ShapeDtypeStruct((col_blocks, width), jnp.float32),
            ),
            in_specs=[smem, smem, smem, pl.BlockSpec(memory_space=pl.ANY)],
            out_specs=(vmem, vmem),
            scratch_shapes=[
                pltpu.VMEM((slots, width, width), jnp.bfloat16),
                pltpu.VMEM((width, LANES), jnp.bfloat16),
                pltpu.VMEM((col_blocks, width), jnp.float32),
                pltpu.VMEM((2, width, LANES), jnp.float32),
                pltpu.VMEM((2, width, LANES), jnp.float32),
                pltpu.VMEM((2, width, LANES), jnp.float32),
                pltpu.VMEM((2, width, LANES), jnp.float32),
                pltpu.VMEM((SWEEPS, BR_DEV, width), jnp.float32),
                pltpu.VMEM((SWEEPS, n_pcol - 1, BR_DEV, width), jnp.float32),
                pltpu.VMEM((SWEEPS, share, width), jnp.float32),
                pltpu.VMEM((SWEEPS, n_pcol, share, width), jnp.float32),
                pltpu.VMEM((SWEEPS, col_blocks, width), jnp.float32),
                pltpu.VMEM((SWEEPS, n_prow - 1, col_blocks, width), jnp.float32),
                pltpu.SemaphoreType.DMA((slots // STEP,)),
                pltpu.SemaphoreType.DMA((SWEEPS, n_pcol - 1)),
                pltpu.SemaphoreType.DMA((SWEEPS, n_pcol - 1)),
                pltpu.SemaphoreType.DMA((SWEEPS, n_pcol - 1)),
                pltpu.SemaphoreType.DMA((SWEEPS, n_pcol - 1)),
                pltpu.SemaphoreType.DMA((SWEEPS, n_prow - 1)),
                pltpu.SemaphoreType.DMA((SWEEPS, n_prow - 1)),
            ],
            compiler_params=pltpu.CompilerParams(collective_id=0, has_side_effects=True),
        )(
            tile_brow.reshape(slots), tile_bcol.reshape(slots), tile_count.reshape(1),
            tiles.reshape(slots, width, width),
        )
        return pl.pallas_call(
            spell,
            out_shape=(
                jax.ShapeDtypeStruct((BR_DEV, 1, width), jnp.float32),
                jax.ShapeDtypeStruct((col_blocks, 1, width), jnp.float32),
            ),
            in_specs=[vmem, vmem],
            out_specs=(vmem, vmem),
        )(row_vec, col_vec)

    return jax.shard_map(
        on_device,
        mesh=mesh,
        in_specs=(
            P("prow", "pcol", None, None, None),
            P("prow", "pcol", None),
            P("prow", "pcol", None),
            P("prow", "pcol"),
        ),
        out_specs=(P(None, "prow", None), P(None, "pcol", None)),
        check_vma=False,
    )
```
